8 devices in a mesh: dp: 1 (over z), pz: 2 (over y), py: 2 (over x), px: 2 (over core).
Axes of the slice: x: 2, y: 2, z: 1, core: 2. Of those that a mesh axis runs over, the one named last changes fastest.
Arguments:
- volumes: bfloat16 [2, 32, 128, 128, 128], P('dp', None, 'px', 'py', 'pz')
- filter_taps: float32 [3, 3, 15], replicated
- mix_weight: bfloat16 [3, 32, 32], replicated
- mix_bias: float32 [3, 32], replicated
Outputs:
- output: bfloat16 [2, 32, 128, 128, 128], P('dp', None, 'px', 'py', 'pz')
All inputs are finite; a program needn't handle non-finite values.
Results may differ from the reference program's by a relative error of at most 0.00422.
Values are sent between devices in bfloat16 or wider.
A program may use at most 1 GiB of HBM per device.

```python
import jax
import jax.numpy as jnp
from jax import lax

CHANNELS = 32
TAPS = 15
LAYERS = 3
VOLUMES = 2
EXTENT_X = 128
EXTENT_Y = 128
EXTENT_Z = 128
HALF_WIDTH = (TAPS - 1) // 2


def setup_inputs(seed: int = 0, part: int = 0) -> dict:
    root_key = jax.random.key(seed)
    key_vol, key_sign, key_mag, key_mix, key_bias = jax.random.split(root_key, 5)
    vol_key = jax.random.fold_in(key_vol, part)
    volumes = jax.random.normal(vol_key, (VOLUMES, CHANNELS, EXTENT_X, EXTENT_Y, EXTENT_Z), jnp.float32).astype(jnp.bfloat16)
    tap_signs = jax.random.bernoulli(key_sign, 0.5, (LAYERS, 3, TAPS)).astype(jnp.float32) * 2.0 - 1.0
    tap_sizes = jax.random.uniform(key_mag, (LAYERS, 3, TAPS), jnp.float32, 0.5, 1.5)
    raw_taps = tap_signs * tap_sizes
    filter_taps = raw_taps / jnp.sqrt(jnp.sum(raw_taps * raw_taps, axis=-1, keepdims=True))
    mix_weight = (jax.random.normal(key_mix, (LAYERS, CHANNELS, CHANNELS), jnp.float32) * CHANNELS ** -0.5).astype(jnp.bfloat16)
    mix_bias = 0.5 * jax.random.normal(key_bias, (LAYERS, CHANNELS), jnp.float32)
    return {'volumes': volumes, 'filter_taps': filter_taps, 'mix_weight': mix_weight, 'mix_bias': mix_bias}


def line_filter(field_3d, tap_row, axis_dim):
    extent = field_3d.shape[axis_dim]
    pad_spec = [(0, 0), (0, 0), (0, 0)]
    pad_spec[axis_dim] = (HALF_WIDTH, HALF_WIDTH)
    padded = jnp.pad(field_3d.astype(jnp.float32), pad_spec)
    taps_used = tap_row.astype(jnp.bfloat16).astype(jnp.float32)
    acc_sum = jnp.zeros(field_3d.shape, jnp.float32)
    for offset in range(TAPS):
        acc_sum = acc_sum + taps_used[offset] * lax.slice_in_dim(padded, offset, offset + extent, axis=axis_dim)
    return acc_sum.astype(jnp.bfloat16)


def layer_step(vol_state, layer_params):
    tap_block, weight, bias_row = layer_params

    def one_volume(volume):
        def one_channel(field_3d):
            field_3d = line_filter(field_3d, tap_block[0], 0)
            field_3d = line_filter(field_3d, tap_block[1], 1)
            return line_filter(field_3d, tap_block[2], 2)

        filtered = lax.map(one_channel, volume)
        flat_units = filtered.reshape(CHANNELS, -1)
        mix_out = jnp.dot(weight.T, flat_units, preferred_element_type=jnp.float32).reshape(volume.shape)
        activated = jax.nn.gelu(mix_out + bias_row[:, None, None, None], approximate=True)
        return (volume.astype(jnp.float32) + activated).astype(jnp.bfloat16)

    return lax.map(one_volume, vol_state), None


def reference(volumes, filter_taps, mix_weight, mix_bias):
    outcome = lax.scan(layer_step, volumes, (filter_taps, mix_weight, mix_bias))
    return outcome[0]
```

```python
import functools

import jax
import jax.numpy as jnp
from jax import lax
from jax.experimental import pallas as pl
from jax.experimental.pallas import tpu as pltpu
from jax.sharding import PartitionSpec as P

SWAP = [(0, 1), (1, 0)]
DIAG = [(0, 3), (1, 2), (2, 1), (3, 0)]
SUB = 16
GROUPS = 4
LANES = 128
PARAMS = pltpu.CompilerParams(vmem_limit_bytes=60 * 1024 * 1024)


def band(taps, offset):
    out = jnp.zeros(taps.shape[:-1] + offset.shape, jnp.float32)
    for t in range(taps.shape[-1]):
        out = out + jnp.where(offset == t, taps[..., t].reshape(taps.shape[:-1] + (1,) * offset.ndim), 0.0)
    return out


def pass_i_weights(taps):
    half = (taps.shape[-1] - 1) // 2
    row = lax.broadcasted_iota(jnp.int32, (8 * SUB, 16 * SUB), 0)
    col = lax.broadcasted_iota(jnp.int32, (8 * SUB, 16 * SUB), 1)
    own, up = col < 8 * SUB, col < 12 * SUB
    point = jnp.where(own, col // SUB, (col % (4 * SUB)) // 8)
    source = jnp.where(own, col % SUB, jnp.where(up, SUB + col % 8, col % 8 - 8))
    offset = jnp.where(row // SUB == point, source - row % SUB + half, -1)
    return band(taps, offset).astype(jnp.bfloat16)


def pass_jk_weights(taps, side):
    half = (taps.shape[-1] - 1) // 2
    shape = (3, SUB, 2 * SUB)
    variant = lax.broadcasted_iota(jnp.int32, shape, 0)
    out = lax.broadcasted_iota(jnp.int32, shape, 1)
    slot = lax.broadcasted_iota(jnp.int32, shape, 2)
    missing_low = (variant == 0) & (slot < half) & (side == 0)
    missing_high = (variant == 2) & (slot >= SUB + half) & (side == 1)
    small = band(taps, jnp.where(missing_low | missing_high, -1, slot - out)).astype(jnp.bfloat16)
    rows, cols = SUB * SUB, 2 * SUB * SUB
    spread_rows = (jnp.arange(rows)[:, None] // SUB == jnp.arange(SUB)[None, :]).astype(jnp.bfloat16)
    spread_cols = (jnp.arange(2 * SUB)[:, None] == jnp.arange(cols)[None, :] // SUB).astype(jnp.bfloat16)
    same = jnp.arange(rows)[:, None] % SUB == jnp.arange(cols)[None, :] % SUB
    tall = jnp.einsum('ra,lvas->lvrs', spread_rows, small, preferred_element_type=jnp.float32).astype(jnp.bfloat16)
    wide = jnp.einsum('lvrs,sc->lvrc', tall, spread_cols, preferred_element_type=jnp.float32)
    return jnp.where(same, wide, 0.0).astype(jnp.bfloat16)


def pass_i_kernel(flags, w_ref, y_ref, n_ref, o_ref):
    jb, kk = y_ref.shape[0], y_ref.shape[1]
    lane = lax.broadcasted_iota(jnp.int32, (1, SUB, LANES), 2)
    has_up, has_low = flags[0] > 0, flags[1] > 0
    weights = w_ref[...]
    zero = jnp.zeros((4, SUB, LANES), jnp.bfloat16)
    width = LANES // GROUPS

    def columns(j, k):
        own = y_ref[j, pl.ds(k, 8)]
        full = own.astype(jnp.float32)
        peer = n_ref[j, pl.ds(k // 2, 4)]
        lo = full[:, :8].reshape(4, SUB, LANES).astype(jnp.bfloat16)
        hi = full[:, 8:].reshape(4, SUB, LANES).astype(jnp.bfloat16)
        up = jnp.where(lane < width, jnp.where(has_up, peer, zero), lo)
        low = jnp.where(lane >= LANES - width, jnp.where(has_low, peer, zero), hi)
        up = pltpu.roll(up, LANES - width, 2)
        low = pltpu.roll(low, width, 2)
        return jnp.concatenate([own.reshape(8 * SUB, LANES), up.reshape(4 * SUB, LANES), low.reshape(4 * SUB, LANES)], axis=0)

    group = 4

    def step(q, carry):
        for r in range(group):
            j = q * group + r
            stacks = [jnp.concatenate([columns(j, k), columns(j, k + 8)], axis=1) for k in range(0, kk, 16)]
            for stack, k in zip(stacks, range(0, kk, 16)):
                out = jnp.dot(weights, stack, preferred_element_type=jnp.float32).astype(jnp.bfloat16)
                o_ref[j, pl.ds(k, 8)] = out[:, :LANES].reshape(8, SUB, LANES)
                o_ref[j, pl.ds(k + 8, 8)] = out[:, LANES:].reshape(8, SUB, LANES)
        return carry

    lax.fori_loop(0, jb // group, step, 0)


def pass_i(flags, weights, y, peer, block=8):
    nj, nk = y.shape[0], y.shape[1]
    return pl.pallas_call(
        pass_i_kernel,
        out_shape=jax.ShapeDtypeStruct(y.shape, y.dtype),
        grid=(nj // block,),
        in_specs=[
            pl.BlockSpec(memory_space=pltpu.SMEM),
            pl.BlockSpec(weights.shape, lambda b: (0, 0)),
            pl.BlockSpec((block, nk, SUB, LANES), lambda b: (b, 0, 0, 0)),
            pl.BlockSpec((block, nk // 2, SUB, LANES), lambda b: (b, 0, 0, 0)),
        ],
        out_specs=pl.BlockSpec((block, nk, SUB, LANES), lambda b: (b, 0, 0, 0)),
        compiler_params=PARAMS,
        cost_estimate=pl.CostEstimate(flops=nj * nk * 2 * SUB * 32 * 8 * LANES, bytes_accessed=nj * nk * 10240, transcendentals=0),
        name="pass_i",
    )(flags, weights, y, peer)


def slots(part, own, halo, n, half):
    lo, hi = part * SUB - half, part * SUB - half + 2 * SUB
    pieces = []
    if lo < 0:
        pieces.append(halo(slice(0, -lo)))
    pieces.append(own(slice(max(lo, 0), min(hi, n))))
    if hi > n:
        pieces.append(halo(slice(0, half)))
        if hi - n > half:
            pieces.append(halo(slice(0, hi - n - half)))
    stack = jnp.concatenate(pieces, axis=0) if len(pieces) > 1 else pieces[0]
    return stack.reshape(2 * SUB * SUB, LANES)


def pass_j_kernel(w_ref, u_ref, h_ref, o_ref):
    nj, kb = u_ref.shape[0], u_ref.shape[1]
    half = h_ref.shape[0]
    parts = nj // SUB

    def pair(k0, k1):
        for part in range(parts):
            sides = [slots(part, lambda s, k=k: u_ref[s, k], lambda s, k=k: h_ref[s, k], nj, half) for k in (k0, k1)]
            variant = 0 if part == 0 else (2 if part == parts - 1 else 1)
            out = jnp.dot(w_ref[variant], jnp.concatenate(sides, axis=1), preferred_element_type=jnp.float32).astype(jnp.bfloat16)
            o_ref[part * SUB:(part + 1) * SUB, k0] = out[:, :LANES].reshape(SUB, SUB, LANES)
            o_ref[part * SUB:(part + 1) * SUB, k1] = out[:, LANES:].reshape(SUB, SUB, LANES)

    for q in range((kb + 1) // 2):
        pair(2 * q, min(2 * q + 1, kb - 1))


def pass_j(weights, u, halo, block):
    nj, nk = u.shape[0], u.shape[1]
    return pl.pallas_call(
        pass_j_kernel,
        out_shape=jax.ShapeDtypeStruct(u.shape, u.dtype),
        grid=(nk // block,),
        in_specs=[
            pl.BlockSpec(weights.shape, lambda b: (0, 0, 0)),
            pl.BlockSpec((nj, block, SUB, LANES), lambda b: (0, b, 0, 0)),
            pl.BlockSpec((halo.shape[0], block, SUB, LANES), lambda b: (0, b, 0, 0)),
        ],
        out_specs=pl.BlockSpec((nj, block, SUB, LANES), lambda b: (0, b, 0, 0)),
        compiler_params=PARAMS,
        cost_estimate=pl.CostEstimate(flops=nj * nk * 2 * SUB * 512 * LANES, bytes_accessed=nj * nk * 8192, transcendentals=0),
        name="pass_j",
    )(weights, u, halo)


def gelu_tanh(x):
    inner = x * (0.7978845608028654 + (0.7978845608028654 * 0.044715) * (x * x))
    half_x = 0.5 * x
    return half_x + half_x * jnp.tanh(inner)


def pass_k_kernel(flags, w_ref, m_ref, b_ref, u_ref, h_ref, y_ref, o_ref, f_ref):
    jb, nk = u_ref.shape[0], u_ref.shape[1]
    half = h_ref.shape[1]
    parts = nk // SUB
    send_high = flags[0] > 0
    rows = 128
    tiles = rows // SUB

    def filtered(j0, part):
        sides = [slots(part, lambda s, j=j: u_ref[j, s], lambda s, j=j: h_ref[j, s], nk, half) for j in (j0, j0 + 1)]
        variant = 0 if part == 0 else (2 if part == parts - 1 else 1)
        return jnp.dot(w_ref[variant], jnp.concatenate(sides, axis=1), preferred_element_type=jnp.float32).astype(jnp.bfloat16)

    def finish(j0, part, u3):
        for r in range(SUB * SUB // rows):
            z = jnp.dot(u3[r * rows:(r + 1) * rows], m_ref[...], preferred_element_type=jnp.float32) + b_ref[...]
            act = gelu_tanh(z)
            k0 = part * SUB + r * tiles
            for side in range(2):
                new = y_ref[j0 + side, k0:k0 + tiles].astype(jnp.float32) + act[:, side * LANES:(side + 1) * LANES].reshape(tiles, SUB, LANES)
                o_ref[j0 + side, k0:k0 + tiles] = new.astype(jnp.bfloat16)
                face = jnp.where(send_high, new[:, 8:], new[:, :8])
                f_ref[j0 + side, k0 // 2:(k0 + tiles) // 2] = face.reshape(tiles // 2, SUB, LANES).astype(jnp.bfloat16)

    def step(q, carry):
        waiting = []
        for j0 in (4 * q, 4 * q + 2):
            for part in range(parts):
                waiting.append((j0, part, filtered(j0, part)))
                if len(waiting) > 2:
                    finish(*waiting.pop(0))
        for item in waiting:
            finish(*item)
        return carry

    lax.fori_loop(0, jb // 4, step, 0)


def pass_k(flags, weights, mix, bias, u, halo, y, block=4):
    nj, nk = u.shape[0], u.shape[1]
    return pl.pallas_call(
        pass_k_kernel,
        out_shape=(jax.ShapeDtypeStruct(u.shape, u.dtype), jax.ShapeDtypeStruct((nj, nk // 2, SUB, LANES), u.dtype)),
        grid=(nj // block,),
        in_specs=[
            pl.BlockSpec(memory_space=pltpu.SMEM),
            pl.BlockSpec(weights.shape, lambda b: (0, 0, 0)),
            pl.BlockSpec(mix.shape, lambda b: (0, 0)),
            pl.BlockSpec(bias.shape, lambda b: (0, 0)),
            pl.BlockSpec((block, nk, SUB, LANES), lambda b: (b, 0, 0, 0)),
            pl.BlockSpec((block, halo.shape[1], SUB, LANES), lambda b: (b, 0, 0, 0)),
            pl.BlockSpec((block, nk, SUB, LANES), lambda b: (b, 0, 0, 0)),
        ],
        out_specs=(
            pl.BlockSpec((block, nk, SUB, LANES), lambda b: (b, 0, 0, 0)),
            pl.BlockSpec((block, nk // 2, SUB, LANES), lambda b: (b, 0, 0, 0)),
        ),
        compiler_params=PARAMS,
        cost_estimate=pl.CostEstimate(flops=nj * nk * 2 * SUB * (512 + 256) * LANES, bytes_accessed=nj * nk * 14336, transcendentals=nj * nk * SUB * LANES),
        name="pass_k_mix",
    )(flags, weights, mix, bias, u, halo, y)


PITCH = 24


def enter_kernel(flags, x_ref, o_ref, f_ref, s1, s2):
    nc, nk = x_ref.shape[1], x_ref.shape[4]
    rows = GROUPS * nc
    send_high = flags[0] > 0

    def pair(p, carry):
        for g in range(GROUPS):
            for c in range(nc):
                i0 = g * SUB + 2 * p
                tile = jnp.concatenate([x_ref[0, c, i0], x_ref[0, c, i0 + 1]], axis=1)
                s1[(g * nc + c) * PITCH:(g * nc + c) * PITCH + SUB, :] = tile.astype(jnp.float32)
        for j in range(SUB):
            flip = s1[pl.ds(j, rows, stride=PITCH), :].T
            base = j * nk * PITCH + 2 * p
            s2[pl.ds(base, nk, stride=PITCH), :] = flip[:nk]
            s2[pl.ds(base + 1, nk, stride=PITCH), :] = flip[nk:]
        return carry

    lax.fori_loop(0, SUB // 2, pair, 0)

    def emit(j, carry):
        base = pl.multiple_of(j * (nk * PITCH), 8)
        for k in range(0, nk, 2):
            faces = []
            for side in range(2):
                tile = s2[pl.ds(base + (k + side) * PITCH, SUB), :]
                o_ref[j, k + side] = tile.astype(jnp.bfloat16)
                faces.append(jnp.where(send_high, tile[8:], tile[:8]))
            f_ref[j, k // 2] = jnp.concatenate(faces, axis=0).astype(jnp.bfloat16)
        return carry

    lax.fori_loop(0, SUB, emit, 0)


def enter(flags, vol, v):
    nv, nc, ni, nj, nk = vol.shape
    return pl.pallas_call(
        enter_kernel,
        out_shape=(jax.ShapeDtypeStruct((nj, nk, SUB, LANES), vol.dtype), jax.ShapeDtypeStruct((nj, nk // 2, SUB, LANES), vol.dtype)),
        grid=(nj // SUB,),
        in_specs=[pl.BlockSpec(memory_space=pltpu.SMEM), pl.BlockSpec((1, nc, ni, SUB, nk), lambda b: (v, 0, 0, b, 0))],
        out_specs=(
            pl.BlockSpec((SUB, nk, SUB, LANES), lambda b: (b, 0, 0, 0)),
            pl.BlockSpec((SUB, nk // 2, SUB, LANES), lambda b: (b, 0, 0, 0)),
        ),
        scratch_shapes=[pltpu.VMEM((GROUPS * nc * PITCH, 2 * nk), jnp.float32), pltpu.VMEM((SUB * nk * PITCH, LANES), jnp.float32)],
        compiler_params=PARAMS,
        cost_estimate=pl.CostEstimate(flops=10**8, bytes_accessed=nj * nk * 12288, transcendentals=0),
        name="enter",
    )(flags, vol)


def leave_kernel(y_ref, *rest):
    o_ref, s1, s2 = rest[-3:]
    nc, nk = o_ref.shape[1], o_ref.shape[4]
    rows = GROUPS * nc

    def take(j, carry):
        base = pl.multiple_of(j * (nk * PITCH), 8)
        for k in range(nk):
            s2[pl.ds(base + k * PITCH, SUB), :] = y_ref[j, k].astype(jnp.float32)
        return carry

    lax.fori_loop(0, SUB, take, 0)

    def pair(p, carry):
        for j in range(SUB):
            base = j * nk * PITCH + 2 * p
            both = jnp.concatenate([s2[pl.ds(base, nk, stride=PITCH), :], s2[pl.ds(base + 1, nk, stride=PITCH), :]], axis=0)
            s1[pl.ds(j, rows, stride=PITCH), :] = both.T
        for g in range(GROUPS):
            for c in range(nc):
                i0 = g * SUB + 2 * p
                tile = s1[(g * nc + c) * PITCH:(g * nc + c) * PITCH + SUB, :].astype(jnp.bfloat16)
                o_ref[0, c, i0] = tile[:, :nk]
                o_ref[0, c, i0 + 1] = tile[:, nk:]
        return carry

    lax.fori_loop(0, SUB // 2, pair, 0)


def leave(y, v, shape, previous):
    nv, nc, ni, nj, nk = shape
    extra = [] if previous is None else [previous]
    return pl.pallas_call(
        leave_kernel,
        out_shape=jax.ShapeDtypeStruct(shape, y.dtype),
        grid=(nj // SUB,),
        in_specs=[pl.BlockSpec((SUB, nk, SUB, LANES), lambda b: (b, 0, 0, 0))] + [pl.BlockSpec(memory_space=pl.ANY)] * len(extra),
        out_specs=pl.BlockSpec((1, nc, ni, SUB, nk), lambda b: (v, 0, 0, b, 0)),
        scratch_shapes=[pltpu.VMEM((GROUPS * nc * PITCH, 2 * nk), jnp.float32), pltpu.VMEM((SUB * nk * PITCH, LANES), jnp.float32)],
        input_output_aliases={1: 0} if extra else {},
        compiler_params=PARAMS,
        cost_estimate=pl.CostEstimate(flops=10**8, bytes_accessed=nj * nk * 12288, transcendentals=0),
        name="leave",
    )(y, *extra)


def solution(mesh):
    vol_spec = P('dp', None, 'px', 'py', 'pz')

    def local_layers(vol_block, filter_taps, mix_weight, mix_bias):
        nv, nc, ni, nj, nk = vol_block.shape
        layers = filter_taps.shape[0]
        half = (filter_taps.shape[2] - 1) // 2
        px, py, pz = lax.axis_index('px'), lax.axis_index('py'), lax.axis_index('pz')
        taps = filter_taps.astype(jnp.bfloat16).astype(jnp.float32)
        w_i = pass_i_weights(taps[:, 0])
        w_j = pass_jk_weights(taps[:, 1], py)
        w_k = pass_jk_weights(taps[:, 2], pz)
        eye = jnp.eye(2 * GROUPS, dtype=jnp.bfloat16)
        mix = (eye[None, :, None, :, None] * mix_weight[:, None, :, None, :]).reshape(layers, 2 * LANES, 2 * LANES)
        bias = jnp.tile(mix_bias, (1, 2 * GROUPS)).reshape(layers, 1, 2 * LANES)
        flags_x = jnp.stack([px == 0, px == 1]).astype(jnp.int32)
        j_at = jnp.where(py == 0, nj - half, 0)
        k_at = jnp.where(pz == 0, nk - half, 0)

        state, peers = [], []
        for v in range(nv):
            y, face = enter(flags_x, vol_block, v)
            state.append(y)
            peers.append(lax.ppermute(face, 'px', SWAP))
        for layer in range(layers):
            firsts = []
            for v in range(nv):
                u1 = pass_i(flags_x, w_i[layer], state[v], peers[v])
                j_face = lax.dynamic_slice_in_dim(u1, j_at, half, axis=0)
                k_face = lax.dynamic_slice_in_dim(u1, k_at, half, axis=1)
                corner = lax.dynamic_slice_in_dim(j_face, k_at, half, axis=1)
                firsts.append((
                    u1,
                    lax.ppermute(j_face, 'py', SWAP),
                    lax.ppermute(k_face, 'pz', SWAP),
                    lax.ppermute(corner, ('pz', 'py'), DIAG),
                ))
            for v in range(nv):
                u1, j_halo, k_halo, corner = firsts[v]
                u2 = pass_j(w_j[layer], u1, j_halo, 16)
                u2_halo = pass_j(w_j[layer], k_halo, corner, half)
                state[v], face = pass_k(flags_x, w_k[layer], mix[layer], bias[layer], u2, u2_halo, state[v])
                if layer + 1 < layers:
                    peers[v] = lax.ppermute(face, 'px', SWAP)
        out = None
        for v in range(nv):
            out = leave(state[v], v, vol_block.shape, out)
        return out

    return jax.shard_map(local_layers, mesh=mesh, in_specs=(vol_spec, P(), P(), P()), out_specs=vol_spec, check_vma=False)
```

```python
import jax
import jax.numpy as jnp
from jax import lax
from jax.experimental import pallas as pl
from jax.experimental.pallas import tpu as pltpu
from jax.sharding import PartitionSpec as P


SWAP = [(0, 1), (1, 0)]
DIAG = [(0, 3), (1, 2), (2, 1), (3, 0)]
SUB = 16
GROUPS = 4
LANES = 128
PARAMS = pltpu.CompilerParams(vmem_limit_bytes=60 * 1024 * 1024)


def band(taps, offset):
    out = jnp.zeros(taps.shape[:-1] + offset.shape, jnp.float32)
    for t in range(taps.shape[-1]):
        out = out + jnp.where(offset == t, taps[..., t].reshape(taps.shape[:-1] + (1,) * offset.ndim), 0.0)
    return out


def pass_i_weights(taps):
    half = (taps.shape[-1] - 1) // 2
    row = lax.broadcasted_iota(jnp.int32, (8 * SUB, 16 * SUB), 0)
    col = lax.broadcasted_iota(jnp.int32, (8 * SUB, 16 * SUB), 1)
    own, up = col < 8 * SUB, col < 12 * SUB
    point = jnp.where(own, col // SUB, (col % (4 * SUB)) // 8)
    source = jnp.where(own, col % SUB, jnp.where(up, SUB + col % 8, col % 8 - 8))
    offset = jnp.where(row // SUB == point, source - row % SUB + half, -1)
    return band(taps, offset).astype(jnp.bfloat16)


def pass_jk_weights(taps, side):
    half = (taps.shape[-1] - 1) // 2
    shape = (3, SUB, 2 * SUB)
    variant = lax.broadcasted_iota(jnp.int32, shape, 0)
    out = lax.broadcasted_iota(jnp.int32, shape, 1)
    slot = lax.broadcasted_iota(jnp.int32, shape, 2)
    missing_low = (variant == 0) & (slot < half) & (side == 0)
    missing_high = (variant == 2) & (slot >= SUB + half) & (side == 1)
    small = band(taps, jnp.where(missing_low | missing_high, -1, slot - out)).astype(jnp.bfloat16)
    rows, cols = SUB * SUB, 2 * SUB * SUB
    spread_rows = (jnp.arange(rows)[:, None] // SUB == jnp.arange(SUB)[None, :]).astype(jnp.bfloat16)
    spread_cols = (jnp.arange(2 * SUB)[:, None] == jnp.arange(cols)[None, :] // SUB).astype(jnp.bfloat16)
    same = jnp.arange(rows)[:, None] % SUB == jnp.arange(cols)[None, :] % SUB
    tall = jnp.einsum('ra,lvas->lvrs', spread_rows, small, preferred_element_type=jnp.float32).astype(jnp.bfloat16)
    wide = jnp.einsum('lvrs,sc->lvrc', tall, spread_cols, preferred_element_type=jnp.float32)
    return jnp.where(same, wide, 0.0).astype(jnp.bfloat16)


WIDTH = LANES // GROUPS


def gather_faces(pairs, high):
    lane = lax.broadcasted_iota(jnp.int32, (SUB, LANES), 1)
    out = None
    for q in range(GROUPS):
        moved = pltpu.roll(pairs[q], WIDTH * lax.rem(q + high, GROUPS), 1)
        out = moved if out is None else jnp.where(lane // WIDTH == q, moved, out)
    return out


def pass_i_kernel(flags, w_ref, y_ref, n_ref, o_ref, f_ref):
    jb, kk = y_ref.shape[0], y_ref.shape[1]
    lane = lax.broadcasted_iota(jnp.int32, (1, SUB, LANES), 2)
    has_up, has_low = flags[0] > 0, flags[1] > 0
    weights = w_ref[...]
    zero = jnp.zeros((4, SUB, LANES), jnp.bfloat16)

    def columns(j, k):
        own = y_ref[j, pl.ds(k, 8)]
        full = own.astype(jnp.float32)
        tile = n_ref[j, k // 8]
        peer = jnp.stack([pltpu.roll(tile, WIDTH * lax.rem(2 * GROUPS - q - flags[0], GROUPS), 1) for q in range(GROUPS)])
        lo = full[:, :8].reshape(4, SUB, LANES).astype(jnp.bfloat16)
        hi = full[:, 8:].reshape(4, SUB, LANES).astype(jnp.bfloat16)
        up = jnp.where(lane >= LANES - WIDTH, jnp.where(has_up, peer, zero), pltpu.roll(lo, LANES - WIDTH, 2))
        low = jnp.where(lane < WIDTH, jnp.where(has_low, peer, zero), pltpu.roll(hi, WIDTH, 2))
        return jnp.concatenate([own.reshape(8 * SUB, LANES), up.reshape(4 * SUB, LANES), low.reshape(4 * SUB, LANES)], axis=0)

    group = 4

    def step(q, carry):
        for r in range(group):
            j = q * group + r
            stacks = [jnp.concatenate([columns(j, k), columns(j, k + 8)], axis=1) for k in range(0, kk, 16)]
            for stack, k in zip(stacks, range(0, kk, 16)):
                out = jnp.dot(weights, stack, preferred_element_type=jnp.float32).astype(jnp.bfloat16)
                o_ref[j, pl.ds(k, 8)] = out[:, :LANES].reshape(8, SUB, LANES)
                o_ref[j, pl.ds(k + 8, 8)] = out[:, LANES:].reshape(8, SUB, LANES)
        for r in range(group):
            j = q * group + r
            f_ref[j] = o_ref[j, pl.ds(flags[2], f_ref.shape[1])]
        return carry

    lax.fori_loop(0, jb // group, step, 0)


def pass_i(flags, weights, y, peer, half, block=8):
    nj, nk = y.shape[0], y.shape[1]
    return pl.pallas_call(
        pass_i_kernel,
        out_shape=(jax.ShapeDtypeStruct(y.shape, y.dtype), jax.ShapeDtypeStruct((nj, half, SUB, LANES), y.dtype)),
        grid=(nj // block,),
        in_specs=[
            pl.BlockSpec(memory_space=pltpu.SMEM),
            pl.BlockSpec(weights.shape, lambda b: (0, 0)),
            pl.BlockSpec((block, nk, SUB, LANES), lambda b: (b, 0, 0, 0)),
            pl.BlockSpec((block, nk // 8, SUB, LANES), lambda b: (b, 0, 0, 0)),
        ],
        out_specs=(
            pl.BlockSpec((block, nk, SUB, LANES), lambda b: (b, 0, 0, 0)),
            pl.BlockSpec((block, half, SUB, LANES), lambda b: (b, 0, 0, 0)),
        ),
        compiler_params=PARAMS,
        cost_estimate=pl.CostEstimate(flops=nj * nk * 2 * SUB * 32 * 8 * LANES, bytes_accessed=nj * nk * 10240, transcendentals=0),
        name="pass_i",
    )(flags, weights, y, peer)


def slots(part, own, halo, n, half):
    lo, hi = part * SUB - half, part * SUB - half + 2 * SUB
    pieces = []
    if lo < 0:
        pieces.append(halo(slice(0, -lo)))
    pieces.append(own(slice(max(lo, 0), min(hi, n))))
    if hi > n:
        pieces.append(halo(slice(0, half)))
        if hi - n > half:
            pieces.append(halo(slice(0, hi - n - half)))
    stack = jnp.concatenate(pieces, axis=0) if len(pieces) > 1 else pieces[0]
    return stack.reshape(2 * SUB * SUB, LANES)


def half_gelu(h):
    scale = 0.7978845608028654
    return h + h * jnp.tanh(h * (2.0 * scale + (8.0 * scale * 0.044715) * (h * h)))


def filter_mix_kernel(flags, wj_ref, wk_ref, m_ref, b_ref, u_ref, jh_ref, kh_ref, ch_ref, y_ref, o_ref, f_ref, u2, ahead_a, ahead_b):
    nj, kb = u_ref.shape[0], u_ref.shape[1]
    jb, nk = y_ref.shape[0], y_ref.shape[1]
    half = jh_ref.shape[0]
    first = nk // kb
    now = pl.program_id(0)
    send_high = flags[0] > 0
    rows = 128
    tiles = rows // SUB

    def variant(part, parts):
        return 0 if part == 0 else (2 if part == parts - 1 else 1)

    def along_j(src, halo, pairs, at):
        parts = nj // SUB
        for k0, k1 in pairs:
            for part in range(parts):
                sides = [slots(part, lambda s, k=k: src[s, k], lambda s, k=k: halo[s, k], nj, half) for k in (k0, k1)]
                out = jnp.dot(wj_ref[variant(part, parts)], jnp.concatenate(sides, axis=1), preferred_element_type=jnp.float32).astype(jnp.bfloat16)
                js = slice(part * SUB, (part + 1) * SUB)
                u2[js, at + k0] = out[:, :LANES].reshape(SUB, SUB, LANES)
                u2[js, at + k1] = out[:, LANES:].reshape(SUB, SUB, LANES)

    def along_k(j0, part):
        parts = nk // SUB
        sides = [slots(part, lambda s, j=j: u2[j, s], lambda s, j=j: u2[j, slice(nk + s.start, nk + s.stop)], nk, half) for j in (j0, j0 + 1)]
        return jnp.dot(wk_ref[variant(part, parts)], jnp.concatenate(sides, axis=1), preferred_element_type=jnp.float32).astype(jnp.bfloat16)

    def finish(j0, part, ready):
        for r in range(SUB * SUB // rows):
            h = jnp.dot(ready[part, r * rows:(r + 1) * rows], m_ref[...], preferred_element_type=jnp.float32) + b_ref[...]
            act = half_gelu(h)
            k0 = part * SUB + r * tiles
            for side in range(2):
                new = y_ref[j0 + side, k0:k0 + tiles].astype(jnp.float32) + act[:, side * LANES:(side + 1) * LANES].reshape(tiles, SUB, LANES)
                o_ref[j0 + side, k0:k0 + tiles] = new.astype(jnp.bfloat16)
                face = jnp.where(send_high, new[:, 8:], new[:, :8])
                f_ref[j0 + side, k0 // 8] = gather_faces(face.reshape(tiles // 2, SUB, LANES).astype(jnp.bfloat16), flags[0])

    @pl.when(now == 0)
    def _():
        along_j(kh_ref, ch_ref, [(2 * q, min(2 * q + 1, half - 1)) for q in range((half + 1) // 2)], nk)

    @pl.when(now < first)
    def _():
        def some(q, carry):
            along_j(u_ref, jh_ref, [(4 * q + 2 * r, 4 * q + 2 * r + 1) for r in range(2)], now * kb)
            return carry

        lax.fori_loop(0, kb // 4, some, 0)

    @pl.when(now == first - 1)
    def _():
        for part in range(nk // SUB):
            ahead_a[part] = along_k(0, part)

    @pl.when(now >= first)
    def _():
        base = (now - first) * jb
        for part in range(nk // SUB):
            ahead_b[part] = along_k(base + 2, part)
            finish(0, part, ahead_a)
        following = jnp.minimum(base + 4, nj - 2)
        for part in range(nk // SUB):
            ahead_a[part] = along_k(following, part)
            finish(2, part, ahead_b)


def filter_mix(flags, w_j, w_k, mix, bias, u, j_halo, k_halo, corner, y, kb=16):
    nj, nk = u.shape[0], u.shape[1]
    half = j_halo.shape[0]
    jb = 4
    first = nk // kb
    wide = lambda b: (0, 0, 0, 0)
    columns = lambda b: (0, jnp.minimum(b, first - 1), 0, 0)
    planes = lambda b: (jnp.maximum(b - first, 0), 0, 0, 0)
    return pl.pallas_call(
        filter_mix_kernel,
        out_shape=(jax.ShapeDtypeStruct(u.shape, u.dtype), jax.ShapeDtypeStruct((nj, nk // 8, SUB, LANES), u.dtype)),
        grid=(first + nj // jb,),
        in_specs=[
            pl.BlockSpec(memory_space=pltpu.SMEM),
            pl.BlockSpec(w_j.shape, lambda b: (0, 0, 0)),
            pl.BlockSpec(w_k.shape, lambda b: (0, 0, 0)),
            pl.BlockSpec(mix.shape, lambda b: (0, 0)),
            pl.BlockSpec(bias.shape, lambda b: (0, 0)),
            pl.BlockSpec((nj, kb, SUB, LANES), columns),
            pl.BlockSpec((half, kb, SUB, LANES), columns),
            pl.BlockSpec((nj, half, SUB, LANES), wide),
            pl.BlockSpec((half, half, SUB, LANES), wide),
            pl.BlockSpec((jb, nk, SUB, LANES), planes),
        ],
        out_specs=(
            pl.BlockSpec((jb, nk, SUB, LANES), planes),
            pl.BlockSpec((jb, nk // 8, SUB, LANES), planes),
        ),
        scratch_shapes=[
            pltpu.VMEM((nj, nk + 8, SUB, LANES), u.dtype),
            pltpu.VMEM((nk // SUB, SUB * SUB, 2 * LANES), u.dtype),
            pltpu.VMEM((nk // SUB, SUB * SUB, 2 * LANES), u.dtype),
        ],
        compiler_params=PARAMS,
        cost_estimate=pl.CostEstimate(flops=nj * nk * 2 * SUB * (512 * 2 + 256) * LANES, bytes_accessed=nj * nk * 14336, transcendentals=nj * nk * SUB * LANES),
        name="filter_mix",
    )(flags, w_j, w_k, mix, bias, u, j_halo, k_halo, corner, y)


PITCH = 24


def enter_kernel(flags, x_ref, o_ref, f_ref, s1, s2):
    nc, nk = x_ref.shape[1], x_ref.shape[4]
    rows = GROUPS * nc
    send_high = flags[0] > 0

    def pair(p, carry):
        for g in range(GROUPS):
            for c in range(nc):
                i0 = g * SUB + 2 * p
                tile = jnp.concatenate([x_ref[0, c, i0], x_ref[0, c, i0 + 1]], axis=1)
                s1[(g * nc + c) * PITCH:(g * nc + c) * PITCH + SUB, :] = tile.astype(jnp.float32)
        for j in range(SUB):
            flip = s1[pl.ds(j, rows, stride=PITCH), :].T
            base = j * nk * PITCH + 2 * p
            s2[pl.ds(base, nk, stride=PITCH), :] = flip[:nk]
            s2[pl.ds(base + 1, nk, stride=PITCH), :] = flip[nk:]
        return carry

    lax.fori_loop(0, SUB // 2, pair, 0)

    def emit(j, carry):
        base = pl.multiple_of(j * (nk * PITCH), 8)
        for k in range(0, nk, 8):
            faces = []
            for side in range(8):
                tile = s2[pl.ds(base + (k + side) * PITCH, SUB), :]
                o_ref[j, k + side] = tile.astype(jnp.bfloat16)
                faces.append(jnp.where(send_high, tile[8:], tile[:8]))
            pairs = [jnp.concatenate(faces[2 * q:2 * q + 2], axis=0).astype(jnp.bfloat16) for q in range(GROUPS)]
            f_ref[j, k // 8] = gather_faces(pairs, flags[0])
        return carry

    lax.fori_loop(0, SUB, emit, 0)


def enter(flags, vol, v):
    _, nc, ni, nj, nk = vol.shape
    return pl.pallas_call(
        enter_kernel,
        out_shape=(jax.ShapeDtypeStruct((nj, nk, SUB, LANES), vol.dtype), jax.ShapeDtypeStruct((nj, nk // 8, SUB, LANES), vol.dtype)),
        grid=(nj // SUB,),
        in_specs=[pl.BlockSpec(memory_space=pltpu.SMEM), pl.BlockSpec((1, nc, ni, SUB, nk), lambda b: (v, 0, 0, b, 0))],
        out_specs=(
            pl.BlockSpec((SUB, nk, SUB, LANES), lambda b: (b, 0, 0, 0)),
            pl.BlockSpec((SUB, nk // 8, SUB, LANES), lambda b: (b, 0, 0, 0)),
        ),
        scratch_shapes=[pltpu.VMEM((GROUPS * nc * PITCH, 2 * nk), jnp.float32), pltpu.VMEM((SUB * nk * PITCH, LANES), jnp.float32)],
        compiler_params=PARAMS,
        cost_estimate=pl.CostEstimate(flops=10**8, bytes_accessed=nj * nk * 12288, transcendentals=0),
        name="enter",
    )(flags, vol)


def leave_kernel(y_ref, *rest):
    o_ref, s1, s2 = rest[-3:]
    nc, nk = o_ref.shape[1], o_ref.shape[4]
    rows = GROUPS * nc

    def take(j, carry):
        base = pl.multiple_of(j * (nk * PITCH), 8)
        for k in range(nk):
            s2[pl.ds(base + k * PITCH, SUB), :] = y_ref[j, k].astype(jnp.float32)
        return carry

    lax.fori_loop(0, SUB, take, 0)

    def pair(p, carry):
        for j in range(SUB):
            base = j * nk * PITCH + 2 * p
            both = jnp.concatenate([s2[pl.ds(base, nk, stride=PITCH), :], s2[pl.ds(base + 1, nk, stride=PITCH), :]], axis=0)
            s1[pl.ds(j, rows, stride=PITCH), :] = both.T
        for g in range(GROUPS):
            for c in range(nc):
                i0 = g * SUB + 2 * p
                tile = s1[(g * nc + c) * PITCH:(g * nc + c) * PITCH + SUB, :].astype(jnp.bfloat16)
                o_ref[0, c, i0] = tile[:, :nk]
                o_ref[0, c, i0 + 1] = tile[:, nk:]
        return carry

    lax.fori_loop(0, SUB // 2, pair, 0)


def leave(y, v, shape, previous):
    _, nc, ni, nj, nk = shape
    extra = [] if previous is None else [previous]
    return pl.pallas_call(
        leave_kernel,
        out_shape=jax.ShapeDtypeStruct(shape, y.dtype),
        grid=(nj // SUB,),
        in_specs=[pl.BlockSpec((SUB, nk, SUB, LANES), lambda b: (b, 0, 0, 0))] + [pl.BlockSpec(memory_space=pl.ANY)] * len(extra),
        out_specs=pl.BlockSpec((1, nc, ni, SUB, nk), lambda b: (v, 0, 0, b, 0)),
        scratch_shapes=[pltpu.VMEM((GROUPS * nc * PITCH, 2 * nk), jnp.float32), pltpu.VMEM((SUB * nk * PITCH, LANES), jnp.float32)],
        input_output_aliases={1: 0} if extra else {},
        compiler_params=PARAMS,
        cost_estimate=pl.CostEstimate(flops=10**8, bytes_accessed=nj * nk * 12288, transcendentals=0),
        name="leave",
    )(y, *extra)


def solution(mesh):
    vol_spec = P('dp', None, 'px', 'py', 'pz')

    def local_layers(vol_block, filter_taps, mix_weight, mix_bias):
        nv, _, _, nj, nk = vol_block.shape
        layers = filter_taps.shape[0]
        half = (filter_taps.shape[2] - 1) // 2
        px, py, pz = lax.axis_index('px'), lax.axis_index('py'), lax.axis_index('pz')
        taps = filter_taps.astype(jnp.bfloat16).astype(jnp.float32)
        w_i = pass_i_weights(taps[:, 0])
        w_j = pass_jk_weights(taps[:, 1], py)
        w_k = pass_jk_weights(taps[:, 2], pz)
        eye = jnp.eye(2 * GROUPS, dtype=jnp.bfloat16)
        mix = (eye[None, :, None, :, None] * (0.5 * mix_weight)[:, None, :, None, :]).reshape(layers, 2 * LANES, 2 * LANES)
        bias = jnp.tile(0.5 * mix_bias, (1, 2 * GROUPS)).reshape(layers, 1, 2 * LANES)
        j_at = jnp.where(py == 0, nj - half, 0)
        k_at = jnp.where(pz == 0, nk - half, 0)
        flags_x = jnp.stack([px == 0, px == 1, k_at]).astype(jnp.int32)

        last = [mix]

        def after(value):
            value, _ = lax.optimization_barrier((value, last[0]))
            return value

        def first_half(layer, y, peer):
            u1, k_face = pass_i(flags_x, w_i[layer], after(y), peer, half)
            last[0] = k_face
            j_face = lax.dynamic_slice_in_dim(u1, j_at, half, axis=0)
            corner = lax.dynamic_slice_in_dim(k_face, j_at, half, axis=0)
            j_halo = lax.ppermute(j_face, 'py', SWAP)
            k_halo = lax.ppermute(k_face, 'pz', SWAP)
            corner = lax.ppermute(corner, ('pz', 'py'), DIAG)
            halos = (j_halo, k_halo, corner)
            return u1, halos

        def second_half(layer, y, u1, halos):
            u1 = after(u1)
            y, face = filter_mix(flags_x, w_j[layer], w_k[layer], mix[layer], bias[layer], u1, *halos, y)
            last[0] = face
            return y, lax.ppermute(face, 'px', SWAP) if layer + 1 < layers else None

        def begin(v):
            vol = after(vol_block)
            y, face = enter(flags_x, vol, v)
            last[0] = face
            return y, lax.ppermute(face, 'px', SWAP)

        state = [None] * nv
        firsts = [None] * nv
        for v in range(nv):
            state[v], peer = begin(v)
            firsts[v] = first_half(0, state[v], peer)
        out = None
        for layer in range(layers):
            for v in range(nv):
                state[v], peer = second_half(layer, state[v], *firsts[v])
                if layer + 1 < layers:
                    firsts[v] = first_half(layer + 1, state[v], peer)
                else:
                    out = leave(after(state[v]), v, vol_block.shape, out)
                    last[0] = out
        return out

    return jax.shard_map(local_layers, mesh=mesh, in_specs=(vol_spec, P(), P(), P()), out_specs=vol_spec, check_vma=False)
```

```python
import jax
import jax.numpy as jnp
from jax import lax
from jax.experimental import pallas as pl
from jax.experimental.pallas import tpu as pltpu
from jax.sharding import PartitionSpec as P


SWAP = [(0, 1), (1, 0)]
DIAG = [(0, 3), (1, 2), (2, 1), (3, 0)]
SUB = 16
GROUPS = 4
LANES = 128
PARAMS = pltpu.CompilerParams(vmem_limit_bytes=67043328)


def band(taps, offset):
    out = jnp.zeros(taps.shape[:-1] + offset.shape, jnp.float32)
    for t in range(taps.shape[-1]):
        out = out + jnp.where(offset == t, taps[..., t].reshape(taps.shape[:-1] + (1,) * offset.ndim), 0.0)
    return out


def pass_i_weights(taps):
    half = (taps.shape[-1] - 1) // 2
    row = lax.broadcasted_iota(jnp.int32, (8 * SUB, 16 * SUB), 0)
    col = lax.broadcasted_iota(jnp.int32, (8 * SUB, 16 * SUB), 1)
    own, up = col < 8 * SUB, col < 12 * SUB
    point = jnp.where(own, col // SUB, (col % (4 * SUB)) // 8)
    source = jnp.where(own, col % SUB, jnp.where(up, SUB + col % 8, col % 8 - 8))
    offset = jnp.where(row // SUB == point, source - row % SUB + half, -1)
    return band(taps, offset).astype(jnp.bfloat16)


def pass_jk_weights(taps, side):
    half = (taps.shape[-1] - 1) // 2
    shape = (3, SUB, 2 * SUB)
    variant = lax.broadcasted_iota(jnp.int32, shape, 0)
    out = lax.broadcasted_iota(jnp.int32, shape, 1)
    slot = lax.broadcasted_iota(jnp.int32, shape, 2)
    missing_low = (variant == 0) & (slot < half) & (side == 0)
    missing_high = (variant == 2) & (slot >= SUB + half) & (side == 1)
    small = band(taps, jnp.where(missing_low | missing_high, -1, slot - out)).astype(jnp.bfloat16)
    rows, cols = SUB * SUB, 2 * SUB * SUB
    spread_rows = (jnp.arange(rows)[:, None] // SUB == jnp.arange(SUB)[None, :]).astype(jnp.bfloat16)
    spread_cols = (jnp.arange(2 * SUB)[:, None] == jnp.arange(cols)[None, :] // SUB).astype(jnp.bfloat16)
    same = jnp.arange(rows)[:, None] % SUB == jnp.arange(cols)[None, :] % SUB
    tall = jnp.einsum('ra,lvas->lvrs', spread_rows, small, preferred_element_type=jnp.float32).astype(jnp.bfloat16)
    wide = jnp.einsum('lvrs,sc->lvrc', tall, spread_cols, preferred_element_type=jnp.float32)
    return jnp.where(same, wide, 0.0).astype(jnp.bfloat16)


WIDTH = LANES // GROUPS


def gather_faces(pairs, high):
    lane = lax.broadcasted_iota(jnp.int32, (SUB, LANES), 1)
    out = None
    for q in range(GROUPS):
        moved = pltpu.roll(pairs[q], WIDTH * lax.rem(q + high, GROUPS), 1)
        out = moved if out is None else jnp.where(lane // WIDTH == q, moved, out)
    return out


def pass_i_kernel(flags, w_ref, y_ref, n_ref, o_ref, f_ref, j_ref, c_ref):
    jb, kk = y_ref.shape[0], y_ref.shape[1]
    lane = lax.broadcasted_iota(jnp.int32, (1, SUB, LANES), 2)
    has_up, has_low = flags[0] > 0, flags[1] > 0
    weights = w_ref[...]
    zero = jnp.zeros((4, SUB, LANES), jnp.bfloat16)

    def columns(j, k):
        own = y_ref[j, pl.ds(k, 8)]
        full = own.astype(jnp.float32)
        tile = n_ref[j, k // 8]
        peer = jnp.stack([pltpu.roll(tile, WIDTH * lax.rem(2 * GROUPS - q - flags[0], GROUPS), 1) for q in range(GROUPS)])
        lo = full[:, :8].reshape(4, SUB, LANES).astype(jnp.bfloat16)
        hi = full[:, 8:].reshape(4, SUB, LANES).astype(jnp.bfloat16)
        up = jnp.where(lane >= LANES - WIDTH, jnp.where(has_up, peer, zero), pltpu.roll(lo, LANES - WIDTH, 2))
        low = jnp.where(lane < WIDTH, jnp.where(has_low, peer, zero), pltpu.roll(hi, WIDTH, 2))
        return jnp.concatenate([own.reshape(8 * SUB, LANES), up.reshape(4 * SUB, LANES), low.reshape(4 * SUB, LANES)], axis=0)

    group = 4

    def step(q, carry):
        for r in range(group):
            j = q * group + r
            stacks = [jnp.concatenate([columns(j, k), columns(j, k + 8)], axis=1) for k in range(0, kk, 16)]
            for stack, k in zip(stacks, range(0, kk, 16)):
                out = jnp.dot(weights, stack, preferred_element_type=jnp.float32).astype(jnp.bfloat16)
                o_ref[j, pl.ds(k, 8)] = out[:, :LANES].reshape(8, SUB, LANES)
                o_ref[j, pl.ds(k + 8, 8)] = out[:, LANES:].reshape(8, SUB, LANES)
        for r in range(group):
            j = q * group + r
            f_ref[j] = o_ref[j, pl.ds(flags[2], f_ref.shape[1])]
        return carry

    lax.fori_loop(0, jb // group, step, 0)

    half = j_ref.shape[0]
    at = pl.program_id(0) * jb

    @pl.when((flags[3] >= at) & (flags[3] < at + jb))
    def _():
        def plane(r, carry):
            j_ref[r] = o_ref[flags[3] - at + r]
            c_ref[r] = f_ref[flags[3] - at + r]
            return carry

        lax.fori_loop(0, half, plane, 0)


def pass_i(flags, weights, layer, y, peer, half, block=8):
    nj, nk = y.shape[0], y.shape[1]
    return pl.pallas_call(
        pass_i_kernel,
        out_shape=tuple(jax.ShapeDtypeStruct(lead + (SUB, LANES), y.dtype) for lead in ((nj, nk), (nj, half), (half, nk), (half, half))),
        grid=(nj // block,),
        in_specs=[
            pl.BlockSpec(memory_space=pltpu.SMEM),
            pl.BlockSpec((None,) + weights.shape[1:], lambda b: (layer, 0, 0)),
            pl.BlockSpec((block, nk, SUB, LANES), lambda b: (b, 0, 0, 0)),
            pl.BlockSpec((block, nk // 8, SUB, LANES), lambda b: (b, 0, 0, 0)),
        ],
        out_specs=(
            pl.BlockSpec((block, nk, SUB, LANES), lambda b: (b, 0, 0, 0)),
            pl.BlockSpec((block, half, SUB, LANES), lambda b: (b, 0, 0, 0)),
            pl.BlockSpec((half, nk, SUB, LANES), lambda b: (0, 0, 0, 0)),
            pl.BlockSpec((half, half, SUB, LANES), lambda b: (0, 0, 0, 0)),
        ),
        compiler_params=PARAMS,
        cost_estimate=pl.CostEstimate(flops=nj * nk * 2 * SUB * 32 * 8 * LANES, bytes_accessed=nj * nk * 10240, transcendentals=0),
        name="pass_i",
    )(flags, weights, y, peer)


def slots(part, own, halo, n, half):
    lo, hi = part * SUB - half, part * SUB - half + 2 * SUB
    pieces = []
    if lo < 0:
        pieces.append(halo(slice(0, -lo)))
    pieces.append(own(slice(max(lo, 0), min(hi, n))))
    if hi > n:
        pieces.append(halo(slice(0, half)))
        if hi - n > half:
            pieces.append(halo(slice(0, hi - n - half)))
    stack = jnp.concatenate(pieces, axis=0) if len(pieces) > 1 else pieces[0]
    return stack.reshape(2 * SUB * SUB, LANES)


def half_gelu(h):
    scale = 0.7978845608028654
    return h + h * jnp.tanh(h * (2.0 * scale + (8.0 * scale * 0.044715) * (h * h)))


def filter_mix_kernel(flags, wj_ref, wk_ref, m_ref, b_ref, u_ref, jh_ref, kh_ref, ch_ref, y_ref, o_ref, f_ref, u2, ahead_a, ahead_b):
    nj, kb = u_ref.shape[0], u_ref.shape[1]
    jb, nk = y_ref.shape[0], y_ref.shape[1]
    half = jh_ref.shape[0]
    first = nk // kb
    now = pl.program_id(0)
    send_high = flags[0] > 0
    rows = 128
    tiles = rows // SUB

    def variant(part, parts):
        return 0 if part == 0 else (2 if part == parts - 1 else 1)

    def along_j(src, halo, pairs, at):
        parts = nj // SUB
        for k0, k1 in pairs:
            for part in range(parts):
                sides = [slots(part, lambda s, k=k: src[s, k], lambda s, k=k: halo[s, k], nj, half) for k in (k0, k1)]
                out = jnp.dot(wj_ref[variant(part, parts)], jnp.concatenate(sides, axis=1), preferred_element_type=jnp.float32).astype(jnp.bfloat16)
                js = slice(part * SUB, (part + 1) * SUB)
                u2[js, at + k0] = out[:, :LANES].reshape(SUB, SUB, LANES)
                u2[js, at + k1] = out[:, LANES:].reshape(SUB, SUB, LANES)

    def along_k(j0, part):
        parts = nk // SUB
        sides = [slots(part, lambda s, j=j: u2[j, s], lambda s, j=j: u2[j, slice(nk + s.start, nk + s.stop)], nk, half) for j in (j0, j0 + 1)]
        return jnp.dot(wk_ref[variant(part, parts)], jnp.concatenate(sides, axis=1), preferred_element_type=jnp.float32).astype(jnp.bfloat16)

    def finish(j0, part, ready):
        for r in range(SUB * SUB // rows):
            h = jnp.dot(ready[part, r * rows:(r + 1) * rows], m_ref[...], preferred_element_type=jnp.float32) + b_ref[...]
            act = half_gelu(h)
            k0 = part * SUB + r * tiles
            for side in range(2):
                new = y_ref[j0 + side, k0:k0 + tiles].astype(jnp.float32) + act[:, side * LANES:(side + 1) * LANES].reshape(tiles, SUB, LANES)
                o_ref[j0 + side, k0:k0 + tiles] = new.astype(jnp.bfloat16)
                face = jnp.where(send_high, new[:, 8:], new[:, :8])
                f_ref[j0 + side, k0 // 8] = gather_faces(face.reshape(tiles // 2, SUB, LANES).astype(jnp.bfloat16), flags[0])

    @pl.when(now == 0)
    def _():
        along_j(kh_ref, ch_ref, [(2 * q, min(2 * q + 1, half - 1)) for q in range((half + 1) // 2)], nk)

    @pl.when(now < first)
    def _():
        def some(q, carry):
            along_j(u_ref, jh_ref, [(4 * q + 2 * r, 4 * q + 2 * r + 1) for r in range(2)], now * kb)
            return carry

        lax.fori_loop(0, kb // 4, some, 0)

    @pl.when(now == first - 1)
    def _():
        for part in range(nk // SUB):
            ahead_a[part] = along_k(0, part)

    @pl.when(now >= first)
    def _():
        def four(q, carry):
            base = (now - first) * jb + 4 * q
            for part in range(nk // SUB):
                ahead_b[part] = along_k(base + 2, part)
                finish(4 * q, part, ahead_a)
            following = jnp.minimum(base + 4, nj - 2)
            for part in range(nk // SUB):
                ahead_a[part] = along_k(following, part)
                finish(4 * q + 2, part, ahead_b)
            return carry

        lax.fori_loop(0, jb // 4, four, 0)


def filter_mix(flags, w_j, w_k, mix, bias, layer, u, j_halo, k_halo, corner, y, kb=16):
    nj, nk = u.shape[0], u.shape[1]
    half = j_halo.shape[0]
    jb = 8
    first = nk // kb
    wide = lambda b: (0, 0, 0, 0)
    columns = lambda b: (0, jnp.minimum(b, first - 1), 0, 0)
    planes = lambda b: (jnp.maximum(b - first, 0), 0, 0, 0)
    return pl.pallas_call(
        filter_mix_kernel,
        out_shape=(jax.ShapeDtypeStruct(u.shape, u.dtype), jax.ShapeDtypeStruct((nj, nk // 8, SUB, LANES), u.dtype)),
        grid=(first + nj // jb,),
        in_specs=[
            pl.BlockSpec(memory_space=pltpu.SMEM),
            pl.BlockSpec((None,) + w_j.shape[1:], lambda b: (layer, 0, 0, 0)),
            pl.BlockSpec((None,) + w_k.shape[1:], lambda b: (layer, 0, 0, 0)),
            pl.BlockSpec((None,) + mix.shape[1:], lambda b: (layer, 0, 0)),
            pl.BlockSpec((None,) + bias.shape[1:], lambda b: (layer, 0, 0)),
            pl.BlockSpec((nj, kb, SUB, LANES), columns),
            pl.BlockSpec((half, kb, SUB, LANES), columns),
            pl.BlockSpec((nj, half, SUB, LANES), wide),
            pl.BlockSpec((half, half, SUB, LANES), wide),
            pl.BlockSpec((jb, nk, SUB, LANES), planes),
        ],
        out_specs=(
            pl.BlockSpec((jb, nk, SUB, LANES), planes),
            pl.BlockSpec((jb, nk // 8, SUB, LANES), planes),
        ),
        scratch_shapes=[
            pltpu.VMEM((nj, nk + 8, SUB, LANES), u.dtype),
            pltpu.VMEM((nk // SUB, SUB * SUB, 2 * LANES), u.dtype),
            pltpu.VMEM((nk // SUB, SUB * SUB, 2 * LANES), u.dtype),
        ],
        compiler_params=PARAMS,
        cost_estimate=pl.CostEstimate(flops=nj * nk * 2 * SUB * (512 * 2 + 256) * LANES, bytes_accessed=nj * nk * 14336, transcendentals=nj * nk * SUB * LANES),
        name="filter_mix",
    )(flags, w_j, w_k, mix, bias, u, j_halo, k_halo, corner, y)


PITCH = 24


def enter_kernel(flags, x_ref, o_ref, f_ref, s1, s2):
    nc, nk = x_ref.shape[1], x_ref.shape[4]
    rows = GROUPS * nc
    send_high = flags[0] > 0

    def pair(p, carry):
        for g in range(GROUPS):
            for c in range(nc):
                i0 = g * SUB + 2 * p
                tile = jnp.concatenate([x_ref[0, c, i0], x_ref[0, c, i0 + 1]], axis=1)
                s1[(g * nc + c) * PITCH:(g * nc + c) * PITCH + SUB, :] = tile.astype(jnp.float32)
        for j in range(SUB):
            flip = s1[pl.ds(j, rows, stride=PITCH), :].T
            base = j * nk * PITCH + 2 * p
            s2[pl.ds(base, nk, stride=PITCH), :] = flip[:nk]
            s2[pl.ds(base + 1, nk, stride=PITCH), :] = flip[nk:]
        return carry

    lax.fori_loop(0, SUB // 2, pair, 0)

    def emit(j, carry):
        base = pl.multiple_of(j * (nk * PITCH), 8)
        for k in range(0, nk, 8):
            faces = []
            for side in range(8):
                tile = s2[pl.ds(base + (k + side) * PITCH, SUB), :]
                o_ref[j, k + side] = tile.astype(jnp.bfloat16)
                faces.append(jnp.where(send_high, tile[8:], tile[:8]))
            pairs = [jnp.concatenate(faces[2 * q:2 * q + 2], axis=0).astype(jnp.bfloat16) for q in range(GROUPS)]
            f_ref[j, k // 8] = gather_faces(pairs, flags[0])
        return carry

    lax.fori_loop(0, SUB, emit, 0)


def enter(flags, vol, v):
    _, nc, ni, nj, nk = vol.shape
    return pl.pallas_call(
        enter_kernel,
        out_shape=(jax.ShapeDtypeStruct((nj, nk, SUB, LANES), vol.dtype), jax.ShapeDtypeStruct((nj, nk // 8, SUB, LANES), vol.dtype)),
        grid=(nj // SUB,),
        in_specs=[pl.BlockSpec(memory_space=pltpu.SMEM), pl.BlockSpec((1, nc, ni, SUB, nk), lambda b: (v, 0, 0, b, 0))],
        out_specs=(
            pl.BlockSpec((SUB, nk, SUB, LANES), lambda b: (b, 0, 0, 0)),
            pl.BlockSpec((SUB, nk // 8, SUB, LANES), lambda b: (b, 0, 0, 0)),
        ),
        scratch_shapes=[pltpu.VMEM((GROUPS * nc * PITCH, 2 * nk), jnp.float32), pltpu.VMEM((SUB * nk * PITCH, LANES), jnp.float32)],
        compiler_params=PARAMS,
        cost_estimate=pl.CostEstimate(flops=10**8, bytes_accessed=nj * nk * 12288, transcendentals=0),
        name="enter",
    )(flags, vol)


def leave_kernel(y_ref, *rest):
    o_ref, s1, s2 = rest[-3:]
    nc, nk = o_ref.shape[1], o_ref.shape[4]
    rows = GROUPS * nc

    def take(j, carry):
        base = pl.multiple_of(j * (nk * PITCH), 8)
        for k in range(nk):
            s2[pl.ds(base + k * PITCH, SUB), :] = y_ref[j, k].astype(jnp.float32)
        return carry

    lax.fori_loop(0, SUB, take, 0)

    def pair(p, carry):
        for j in range(SUB):
            base = j * nk * PITCH + 2 * p
            both = jnp.concatenate([s2[pl.ds(base, nk, stride=PITCH), :], s2[pl.ds(base + 1, nk, stride=PITCH), :]], axis=0)
            s1[pl.ds(j, rows, stride=PITCH), :] = both.T
        for g in range(GROUPS):
            for c in range(nc):
                i0 = g * SUB + 2 * p
                tile = s1[(g * nc + c) * PITCH:(g * nc + c) * PITCH + SUB, :].astype(jnp.bfloat16)
                o_ref[0, c, i0] = tile[:, :nk]
                o_ref[0, c, i0 + 1] = tile[:, nk:]
        return carry

    lax.fori_loop(0, SUB // 2, pair, 0)


def leave(y, v, shape, previous):
    _, nc, ni, nj, nk = shape
    extra = [] if previous is None else [previous]
    return pl.pallas_call(
        leave_kernel,
        out_shape=jax.ShapeDtypeStruct(shape, y.dtype),
        grid=(nj // SUB,),
        in_specs=[pl.BlockSpec((SUB, nk, SUB, LANES), lambda b: (b, 0, 0, 0))] + [pl.BlockSpec(memory_space=pl.ANY)] * len(extra),
        out_specs=pl.BlockSpec((1, nc, ni, SUB, nk), lambda b: (v, 0, 0, b, 0)),
        scratch_shapes=[pltpu.VMEM((GROUPS * nc * PITCH, 2 * nk), jnp.float32), pltpu.VMEM((SUB * nk * PITCH, LANES), jnp.float32)],
        input_output_aliases={1: 0} if extra else {},
        compiler_params=PARAMS,
        cost_estimate=pl.CostEstimate(flops=10**8, bytes_accessed=nj * nk * 12288, transcendentals=0),
        name="leave",
    )(y, *extra)


def solution(mesh):
    vol_spec = P('dp', None, 'px', 'py', 'pz')

    def local_layers(vol_block, filter_taps, mix_weight, mix_bias):
        nv, _, _, nj, nk = vol_block.shape
        layers = filter_taps.shape[0]
        half = (filter_taps.shape[2] - 1) // 2
        px, py, pz = lax.axis_index('px'), lax.axis_index('py'), lax.axis_index('pz')
        taps = filter_taps.astype(jnp.bfloat16).astype(jnp.float32)
        w_i = pass_i_weights(taps[:, 0])
        w_j = pass_jk_weights(taps[:, 1], py)
        w_k = pass_jk_weights(taps[:, 2], pz)
        eye = jnp.eye(2 * GROUPS, dtype=jnp.bfloat16)
        mix = (eye[None, :, None, :, None] * (0.5 * mix_weight)[:, None, :, None, :]).reshape(layers, 2 * LANES, 2 * LANES)
        bias = jnp.tile(0.5 * mix_bias, (1, 2 * GROUPS)).reshape(layers, 1, 2 * LANES)
        j_at = jnp.where(py == 0, nj - half, 0)
        k_at = jnp.where(pz == 0, nk - half, 0)
        flags_x = jnp.stack([px == 0, px == 1, k_at, j_at]).astype(jnp.int32)

        last = [mix]

        def after(value):
            value, _ = lax.optimization_barrier((value, last[0]))
            return value

        def first_half(layer, y, peer):
            u1, k_face, j_face, corner = pass_i(flags_x, w_i, layer, after(y), peer, half)
            last[0] = k_face
            j_halo = lax.ppermute(j_face, 'py', SWAP)
            k_halo = lax.ppermute(k_face, 'pz', SWAP)
            corner = lax.ppermute(corner, ('pz', 'py'), DIAG)
            halos = (j_halo, k_halo, corner)
            return u1, halos

        def second_half(layer, y, u1, halos):
            u1 = after(u1)
            y, face = filter_mix(flags_x, w_j, w_k, mix, bias, layer, u1, *halos, y)
            last[0] = face
            return y, lax.ppermute(face, 'px', SWAP) if layer + 1 < layers else None

        def begin(v):
            vol = after(vol_block)
            y, face = enter(flags_x, vol, v)
            last[0] = face
            return y, lax.ppermute(face, 'px', SWAP)

        state = [None] * nv
        firsts = [None] * nv
        for v in range(nv):
            state[v], peer = begin(v)
            firsts[v] = first_half(0, state[v], peer)
        out = None
        for layer in range(layers):
            for v in range(nv):
                state[v], peer = second_half(layer, state[v], *firsts[v])
                if layer + 1 < layers:
                    firsts[v] = first_half(layer + 1, state[v], peer)
                else:
                    out = leave(after(state[v]), v, vol_block.shape, out)
                    last[0] = out
        return out

    return jax.shard_map(local_layers, mesh=mesh, in_specs=(vol_spec, P(), P(), P()), out_specs=vol_spec, check_vma=False)
```

```python
import jax
import jax.numpy as jnp
from jax import lax
from jax.experimental import pallas as pl
from jax.experimental.pallas import tpu as pltpu
from jax.sharding import PartitionSpec as P


SWAP = [(0, 1), (1, 0)]
DIAG = [(0, 3), (1, 2), (2, 1), (3, 0)]
SUB = 16
GROUPS = 4
LANES = 128
PARAMS = pltpu.CompilerParams(vmem_limit_bytes=67043328)


def band(taps, offset):
    out = jnp.zeros(taps.shape[:-1] + offset.shape, jnp.float32)
    for t in range(taps.shape[-1]):
        out = out + jnp.where(offset == t, taps[..., t].reshape(taps.shape[:-1] + (1,) * offset.ndim), 0.0)
    return out


def pass_i_weights(taps):
    half = (taps.shape[-1] - 1) // 2
    row = lax.broadcasted_iota(jnp.int32, (8 * SUB, 16 * SUB), 0)
    col = lax.broadcasted_iota(jnp.int32, (8 * SUB, 16 * SUB), 1)
    own, up = col < 8 * SUB, col < 12 * SUB
    point = jnp.where(own, col // SUB, (col % (4 * SUB)) // 8)
    source = jnp.where(own, col % SUB, jnp.where(up, SUB + col % 8, col % 8 - 8))
    offset = jnp.where(row // SUB == point, source - row % SUB + half, -1)
    return band(taps, offset).astype(jnp.bfloat16)


def pass_jk_weights(taps, side):
    half = (taps.shape[-1] - 1) // 2
    shape = (3, SUB, 2 * SUB)
    variant = lax.broadcasted_iota(jnp.int32, shape, 0)
    out = lax.broadcasted_iota(jnp.int32, shape, 1)
    slot = lax.broadcasted_iota(jnp.int32, shape, 2)
    missing_low = (variant == 0) & (slot < half) & (side == 0)
    missing_high = (variant == 2) & (slot >= SUB + half) & (side == 1)
    small = band(taps, jnp.where(missing_low | missing_high, -1, slot - out)).astype(jnp.bfloat16)
    rows, cols = SUB * SUB, 2 * SUB * SUB
    spread_rows = (jnp.arange(rows)[:, None] // SUB == jnp.arange(SUB)[None, :]).astype(jnp.bfloat16)
    spread_cols = (jnp.arange(2 * SUB)[:, None] == jnp.arange(cols)[None, :] // SUB).astype(jnp.bfloat16)
    same = jnp.arange(rows)[:, None] % SUB == jnp.arange(cols)[None, :] % SUB
    tall = jnp.einsum('ra,lvas->lvrs', spread_rows, small, preferred_element_type=jnp.float32).astype(jnp.bfloat16)
    wide = jnp.einsum('lvrs,sc->lvrc', tall, spread_cols, preferred_element_type=jnp.float32)
    return jnp.where(same, wide, 0.0).astype(jnp.bfloat16)


WIDTH = LANES // GROUPS


def gather_faces(pairs, high):
    lane = lax.broadcasted_iota(jnp.int32, (SUB, LANES), 1)
    out = None
    for q in range(GROUPS):
        moved = pltpu.roll(pairs[q], WIDTH * lax.rem(q + high, GROUPS), 1)
        out = moved if out is None else jnp.where(lane // WIDTH == q, moved, out)
    return out


def pass_i_kernel(flags, w_ref, y_ref, n_ref, o_ref, f_ref, j_ref, c_ref):
    jb, kk = y_ref.shape[0], y_ref.shape[1]
    lane = lax.broadcasted_iota(jnp.int32, (1, SUB, LANES), 2)
    has_up, has_low = flags[0] > 0, flags[1] > 0
    weights = w_ref[...]
    zero = jnp.zeros((4, SUB, LANES), jnp.bfloat16)

    def columns(j, k):
        own = y_ref[j, pl.ds(k, 8)]
        full = own.astype(jnp.float32)
        tile = n_ref[j, k // 8]
        peer = jnp.stack([pltpu.roll(tile, WIDTH * lax.rem(2 * GROUPS - q - flags[0], GROUPS), 1) for q in range(GROUPS)])
        lo = full[:, :8].reshape(4, SUB, LANES).astype(jnp.bfloat16)
        hi = full[:, 8:].reshape(4, SUB, LANES).astype(jnp.bfloat16)
        up = jnp.where(lane >= LANES - WIDTH, jnp.where(has_up, peer, zero), pltpu.roll(lo, LANES - WIDTH, 2))
        low = jnp.where(lane < WIDTH, jnp.where(has_low, peer, zero), pltpu.roll(hi, WIDTH, 2))
        return jnp.concatenate([own.reshape(8 * SUB, LANES), up.reshape(4 * SUB, LANES), low.reshape(4 * SUB, LANES)], axis=0)

    group = 4

    def step(q, carry):
        for r in range(group):
            j = q * group + r
            stacks = [jnp.concatenate([columns(j, k), columns(j, k + 8)], axis=1) for k in range(0, kk, 16)]
            for stack, k in zip(stacks, range(0, kk, 16)):
                out = jnp.dot(weights, stack, preferred_element_type=jnp.float32).astype(jnp.bfloat16)
                o_ref[j, pl.ds(k, 8)] = out[:, :LANES].reshape(8, SUB, LANES)
                o_ref[j, pl.ds(k + 8, 8)] = out[:, LANES:].reshape(8, SUB, LANES)
        for r in range(group):
            j = q * group + r
            f_ref[j] = o_ref[j, pl.ds(flags[2], f_ref.shape[1])]
        return carry

    lax.fori_loop(0, jb // group, step, 0)

    half = j_ref.shape[0]
    at = pl.program_id(0) * jb

    @pl.when((flags[3] >= at) & (flags[3] < at + jb))
    def _():
        def plane(r, carry):
            j_ref[r] = o_ref[flags[3] - at + r]
            c_ref[r] = f_ref[flags[3] - at + r]
            return carry

        lax.fori_loop(0, half, plane, 0)


def pass_i(flags, weights, layer, y, peer, half, block=8):
    nj, nk = y.shape[0], y.shape[1]
    return pl.pallas_call(
        pass_i_kernel,
        out_shape=tuple(jax.ShapeDtypeStruct(lead + (SUB, LANES), y.dtype) for lead in ((nj, nk), (nj, half), (half, nk), (half, half))),
        grid=(nj // block,),
        in_specs=[
            pl.BlockSpec(memory_space=pltpu.SMEM),
            pl.BlockSpec((None,) + weights.shape[1:], lambda b: (layer, 0, 0)),
            pl.BlockSpec((block, nk, SUB, LANES), lambda b: (b, 0, 0, 0)),
            pl.BlockSpec((block, nk // 8, SUB, LANES), lambda b: (b, 0, 0, 0)),
        ],
        out_specs=(
            pl.BlockSpec((block, nk, SUB, LANES), lambda b: (b, 0, 0, 0)),
            pl.BlockSpec((block, half, SUB, LANES), lambda b: (b, 0, 0, 0)),
            pl.BlockSpec((half, nk, SUB, LANES), lambda b: (0, 0, 0, 0)),
            pl.BlockSpec((half, half, SUB, LANES), lambda b: (0, 0, 0, 0)),
        ),
        compiler_params=PARAMS,
        cost_estimate=pl.CostEstimate(flops=nj * nk * 2 * SUB * 32 * 8 * LANES, bytes_accessed=nj * nk * 10240, transcendentals=0),
        name="pass_i",
    )(flags, weights, y, peer)


def slots(part, own, halo, n, half):
    lo, hi = part * SUB - half, part * SUB - half + 2 * SUB
    pieces = []
    if lo < 0:
        pieces.append(halo(slice(0, -lo)))
    pieces.append(own(slice(max(lo, 0), min(hi, n))))
    if hi > n:
        pieces.append(halo(slice(0, half)))
        if hi - n > half:
            pieces.append(halo(slice(0, hi - n - half)))
    stack = jnp.concatenate(pieces, axis=0) if len(pieces) > 1 else pieces[0]
    return stack.reshape(2 * SUB * SUB, LANES)


def half_gelu(h):
    scale = 0.7978845608028654
    return h + h * jnp.tanh(h * (2.0 * scale + (8.0 * scale * 0.044715) * (h * h)))


def filter_mix_kernel(flags, wj_ref, wk_ref, m_ref, b_ref, u_ref, jh_ref, kh_ref, ch_ref, y_ref, o_ref, f_ref, u2, ahead_a, ahead_b):
    nj, kb = u_ref.shape[0], u_ref.shape[1]
    jb, nk = y_ref.shape[0], y_ref.shape[1]
    half = jh_ref.shape[0]
    first = nk // kb
    now = pl.program_id(0)
    send_high = flags[0] > 0
    rows = 128
    tiles = rows // SUB

    def variant(part, parts):
        return 0 if part == 0 else (2 if part == parts - 1 else 1)

    def along_j(src, halo, pairs, at):
        parts = nj // SUB
        for k0, k1 in pairs:
            for part in range(parts):
                sides = [slots(part, lambda s, k=k: src[s, k], lambda s, k=k: halo[s, k], nj, half) for k in (k0, k1)]
                out = jnp.dot(wj_ref[variant(part, parts)], jnp.concatenate(sides, axis=1), preferred_element_type=jnp.float32).astype(jnp.bfloat16)
                js = slice(part * SUB, (part + 1) * SUB)
                u2[js, at + k0] = out[:, :LANES].reshape(SUB, SUB, LANES)
                u2[js, at + k1] = out[:, LANES:].reshape(SUB, SUB, LANES)

    def along_k(j0, part):
        parts = nk // SUB
        sides = [slots(part, lambda s, j=j: u2[j, s], lambda s, j=j: u2[j, slice(nk + s.start, nk + s.stop)], nk, half) for j in (j0, j0 + 1)]
        return jnp.dot(wk_ref[variant(part, parts)], jnp.concatenate(sides, axis=1), preferred_element_type=jnp.float32).astype(jnp.bfloat16)

    def finish(j0, part, ready):
        for r in range(SUB * SUB // rows):
            h = jnp.dot(ready[part, r * rows:(r + 1) * rows], m_ref[...], preferred_element_type=jnp.float32) + b_ref[...]
            act = half_gelu(h)
            k0 = part * SUB + r * tiles
            for side in range(2):
                new = y_ref[j0 + side, k0:k0 + tiles].astype(jnp.float32) + act[:, side * LANES:(side + 1) * LANES].reshape(tiles, SUB, LANES)
                o_ref[j0 + side, k0:k0 + tiles] = new.astype(jnp.bfloat16)
                face = jnp.where(send_high, new[:, 8:], new[:, :8])
                f_ref[j0 + side, k0 // 8] = gather_faces(face.reshape(tiles // 2, SUB, LANES).astype(jnp.bfloat16), flags[0])

    @pl.when(now == 0)
    def _():
        along_j(kh_ref, ch_ref, [(2 * q, min(2 * q + 1, half - 1)) for q in range((half + 1) // 2)], nk)

    @pl.when(now < first)
    def _():
        def some(q, carry):
            along_j(u_ref, jh_ref, [(4 * q + 2 * r, 4 * q + 2 * r + 1) for r in range(2)], now * kb)
            return carry

        lax.fori_loop(0, kb // 4, some, 0)

    @pl.when(now == first - 1)
    def _():
        for part in range(nk // SUB):
            ahead_a[part] = along_k(0, part)

    @pl.when(now >= first)
    def _():
        def four(q, carry):
            base = (now - first) * jb + 4 * q
            for part in range(nk // SUB):
                ahead_b[part] = along_k(base + 2, part)
                finish(4 * q, part, ahead_a)
            following = jnp.minimum(base + 4, nj - 2)
            for part in range(nk // SUB):
                ahead_a[part] = along_k(following, part)
                finish(4 * q + 2, part, ahead_b)
            return carry

        lax.fori_loop(0, jb // 4, four, 0)


def filter_mix(flags, w_j, w_k, mix, bias, layer, u, j_halo, k_halo, corner, y, kb=16):
    nj, nk = u.shape[0], u.shape[1]
    half = j_halo.shape[0]
    jb = 8
    first = nk // kb
    wide = lambda b: (0, 0, 0, 0)
    columns = lambda b: (0, jnp.minimum(b, first - 1), 0, 0)
    planes = lambda b: (jnp.maximum(b - first, 0), 0, 0, 0)
    return pl.pallas_call(
        filter_mix_kernel,
        out_shape=(jax.ShapeDtypeStruct(u.shape, u.dtype), jax.ShapeDtypeStruct((nj, nk // 8, SUB, LANES), u.dtype)),
        grid=(first + nj // jb,),
        in_specs=[
            pl.BlockSpec(memory_space=pltpu.SMEM),
            pl.BlockSpec((None,) + w_j.shape[1:], lambda b: (layer, 0, 0, 0)),
            pl.BlockSpec((None,) + w_k.shape[1:], lambda b: (layer, 0, 0, 0)),
            pl.BlockSpec((None,) + mix.shape[1:], lambda b: (layer, 0, 0)),
            pl.BlockSpec((None,) + bias.shape[1:], lambda b: (layer, 0, 0)),
            pl.BlockSpec((nj, kb, SUB, LANES), columns),
            pl.BlockSpec((half, kb, SUB, LANES), columns),
            pl.BlockSpec((nj, half, SUB, LANES), wide),
            pl.BlockSpec((half, half, SUB, LANES), wide),
            pl.BlockSpec((jb, nk, SUB, LANES), planes),
        ],
        out_specs=(
            pl.BlockSpec((jb, nk, SUB, LANES), planes),
            pl.BlockSpec((jb, nk // 8, SUB, LANES), planes),
        ),
        scratch_shapes=[
            pltpu.VMEM((nj, nk + 8, SUB, LANES), u.dtype),
            pltpu.VMEM((nk // SUB, SUB * SUB, 2 * LANES), u.dtype),
            pltpu.VMEM((nk // SUB, SUB * SUB, 2 * LANES), u.dtype),
        ],
        compiler_params=PARAMS,
        cost_estimate=pl.CostEstimate(flops=nj * nk * 2 * SUB * (512 * 2 + 256) * LANES, bytes_accessed=nj * nk * 14336, transcendentals=nj * nk * SUB * LANES),
        name="filter_mix",
    )(flags, w_j, w_k, mix, bias, u, j_halo, k_halo, corner, y)


PITCH = 24


def enter_kernel(flags, x_ref, o_ref, f_ref, s1, s2):
    nc, nk = x_ref.shape[1], x_ref.shape[4]
    rows = GROUPS * nc
    send_high = flags[0] > 0

    def pair(p, carry):
        for g in range(GROUPS):
            for c in range(nc):
                i0 = g * SUB + 2 * p
                tile = jnp.concatenate([x_ref[0, c, i0], x_ref[0, c, i0 + 1]], axis=1)
                s1[(g * nc + c) * PITCH:(g * nc + c) * PITCH + SUB, :] = tile.astype(jnp.float32)
        for j in range(SUB):
            flip = s1[pl.ds(j, rows, stride=PITCH), :].T
            base = j * nk * PITCH + 2 * p
            s2[pl.ds(base, nk, stride=PITCH), :] = flip[:nk]
            s2[pl.ds(base + 1, nk, stride=PITCH), :] = flip[nk:]
        return carry

    lax.fori_loop(0, SUB // 2, pair, 0)

    def emit(q, carry):
        for r in range(2):
            j = 2 * q + r
            base = pl.multiple_of(j * (nk * PITCH), 8)
            for k in range(0, nk, 8):
                faces = []
                for side in range(8):
                    tile = s2[pl.ds(base + (k + side) * PITCH, SUB), :]
                    o_ref[j, k + side] = tile.astype(jnp.bfloat16)
                    faces.append(jnp.where(send_high, tile[8:], tile[:8]))
                pairs = [jnp.concatenate(faces[2 * t:2 * t + 2], axis=0).astype(jnp.bfloat16) for t in range(GROUPS)]
                f_ref[j, k // 8] = gather_faces(pairs, flags[0])
        return carry

    lax.fori_loop(0, SUB // 2, emit, 0)


def enter(flags, vol, v):
    _, nc, ni, nj, nk = vol.shape
    return pl.pallas_call(
        enter_kernel,
        out_shape=(jax.ShapeDtypeStruct((nj, nk, SUB, LANES), vol.dtype), jax.ShapeDtypeStruct((nj, nk // 8, SUB, LANES), vol.dtype)),
        grid=(nj // SUB,),
        in_specs=[pl.BlockSpec(memory_space=pltpu.SMEM), pl.BlockSpec((1, nc, ni, SUB, nk), lambda b: (v, 0, 0, b, 0))],
        out_specs=(
            pl.BlockSpec((SUB, nk, SUB, LANES), lambda b: (b, 0, 0, 0)),
            pl.BlockSpec((SUB, nk // 8, SUB, LANES), lambda b: (b, 0, 0, 0)),
        ),
        scratch_shapes=[pltpu.VMEM((GROUPS * nc * PITCH, 2 * nk), jnp.float32), pltpu.VMEM((SUB * nk * PITCH, LANES), jnp.float32)],
        compiler_params=PARAMS,
        cost_estimate=pl.CostEstimate(flops=10**8, bytes_accessed=nj * nk * 12288, transcendentals=0),
        name="enter",
    )(flags, vol)


def leave_kernel(y_ref, *rest):
    o_ref, s1, s2 = rest[-3:]
    nc, nk = o_ref.shape[1], o_ref.shape[4]
    rows = GROUPS * nc

    def take(j, carry):
        base = pl.multiple_of(j * (nk * PITCH), 8)
        for k in range(nk):
            s2[pl.ds(base + k * PITCH, SUB), :] = y_ref[j, k].astype(jnp.float32)
        return carry

    lax.fori_loop(0, SUB, take, 0)

    def pair(p, carry):
        for j in range(SUB):
            base = j * nk * PITCH + 2 * p
            both = jnp.concatenate([s2[pl.ds(base, nk, stride=PITCH), :], s2[pl.ds(base + 1, nk, stride=PITCH), :]], axis=0)
            s1[pl.ds(j, rows, stride=PITCH), :] = both.T
        for g in range(GROUPS):
            for c in range(nc):
                i0 = g * SUB + 2 * p
                tile = s1[(g * nc + c) * PITCH:(g * nc + c) * PITCH + SUB, :].astype(jnp.bfloat16)
                o_ref[0, c, i0] = tile[:, :nk]
                o_ref[0, c, i0 + 1] = tile[:, nk:]
        return carry

    lax.fori_loop(0, SUB // 2, pair, 0)


def leave(y, v, shape, previous):
    _, nc, ni, nj, nk = shape
    extra = [] if previous is None else [previous]
    return pl.pallas_call(
        leave_kernel,
        out_shape=jax.ShapeDtypeStruct(shape, y.dtype),
        grid=(nj // SUB,),
        in_specs=[pl.BlockSpec((SUB, nk, SUB, LANES), lambda b: (b, 0, 0, 0))] + [pl.BlockSpec(memory_space=pl.ANY)] * len(extra),
        out_specs=pl.BlockSpec((1, nc, ni, SUB, nk), lambda b: (v, 0, 0, b, 0)),
        scratch_shapes=[pltpu.VMEM((GROUPS * nc * PITCH, 2 * nk), jnp.float32), pltpu.VMEM((SUB * nk * PITCH, LANES), jnp.float32)],
        input_output_aliases={1: 0} if extra else {},
        compiler_params=PARAMS,
        cost_estimate=pl.CostEstimate(flops=10**8, bytes_accessed=nj * nk * 12288, transcendentals=0),
        name="leave",
    )(y, *extra)


def solution(mesh):
    vol_spec = P('dp', None, 'px', 'py', 'pz')

    def local_layers(vol_block, filter_taps, mix_weight, mix_bias):
        nv, _, _, nj, nk = vol_block.shape
        layers = filter_taps.shape[0]
        half = (filter_taps.shape[2] - 1) // 2
        px, py, pz = lax.axis_index('px'), lax.axis_index('py'), lax.axis_index('pz')
        taps = filter_taps.astype(jnp.bfloat16).astype(jnp.float32)
        w_i = pass_i_weights(taps[:, 0])
        w_j = pass_jk_weights(taps[:, 1], py)
        w_k = pass_jk_weights(taps[:, 2], pz)
        eye = jnp.eye(2 * GROUPS, dtype=jnp.bfloat16)
        mix = (eye[None, :, None, :, None] * (0.5 * mix_weight)[:, None, :, None, :]).reshape(layers, 2 * LANES, 2 * LANES)
        bias = jnp.tile(0.5 * mix_bias, (1, 2 * GROUPS)).reshape(layers, 1, 2 * LANES)
        j_at = jnp.where(py == 0, nj - half, 0)
        k_at = jnp.where(pz == 0, nk - half, 0)
        flags_x = jnp.stack([px == 0, px == 1, k_at, j_at]).astype(jnp.int32)

        last = [mix]

        def after(value):
            value, _ = lax.optimization_barrier((value, last[0]))
            return value

        def first_half(layer, y, peer):
            u1, k_face, j_face, corner = pass_i(flags_x, w_i, layer, after(y), peer, half)
            last[0] = k_face
            j_halo = lax.ppermute(j_face, 'py', SWAP)
            k_halo = lax.ppermute(k_face, 'pz', SWAP)
            corner = lax.ppermute(corner, ('pz', 'py'), DIAG)
            halos = (j_halo, k_halo, corner)
            return u1, halos

        def second_half(layer, y, u1, halos):
            u1 = after(u1)
            y, face = filter_mix(flags_x, w_j, w_k, mix, bias, layer, u1, *halos, y)
            last[0] = face
            return y, lax.ppermute(face, 'px', SWAP) if layer + 1 < layers else None

        def begin(v):
            vol = after(vol_block)
            y, face = enter(flags_x, vol, v)
            last[0] = face
            return y, lax.ppermute(face, 'px', SWAP)

        state = [None] * nv
        firsts = [None] * nv
        for v in range(nv):
            state[v], peer = begin(v)
            firsts[v] = first_half(0, state[v], peer)
        out = None
        for layer in range(layers):
            for v in range(nv):
                state[v], peer = second_half(layer, state[v], *firsts[v])
                if layer + 1 < layers:
                    firsts[v] = first_half(layer + 1, state[v], peer)
                else:
                    out = leave(after(state[v]), v, vol_block.shape, out)
                    last[0] = out
        return out

    return jax.shard_map(local_layers, mesh=mesh, in_specs=(vol_spec, P(), P(), P()), out_specs=vol_spec, check_vma=False)
```
